32 devices in a mesh: pool: 2 (over x), seq: 4 (over y, core), head: 4 (over z).
Axes of the slice: x: 2, y: 2, z: 4, core: 2. Of those that a mesh axis runs over, the one named last changes fastest.
Arguments:
- prompt: bfloat16 [8, 2048, 8192], P('pool', 'seq'), may hold values from -6 to 6
- key_value_weight: bfloat16 [8192, 2, 1024], P('seq', None, 'head'), may hold values from -0.0625 to 0.0625
- adapter_down_weight: bfloat16 [8192, 256], P('seq'), may hold values from -0.0625 to 0.0625
- adapter_up_weight: bfloat16 [8, 2, 16, 1024], P(None, None, None, 'head'), may hold values from -0.75 to 0.75
- request_adapter_index: int32 [8], P('pool'), may hold values from 0 to 7
- destination: int32 [8], replicated, may hold values from 0 to 3, as said below
- rotated_query: bfloat16 [384, 8192], P(('pool', 'seq'), 'head'), may hold values from -150 to 150
- key_value_cache: bfloat16 [384, 128, 2, 1024], P(('pool', 'seq'), None, None, 'head'), may hold values from -6 to 6
- current_key_value: bfloat16 [384, 2, 1024], P(('pool', 'seq'), None, 'head'), may hold values from -6 to 6
- cached_length: int32 [384], P(('pool', 'seq')), may hold values from 1 to 128
- row_adapter_index: int32 [384], P('pool'), may hold values from 0 to 7
- output_weight: bfloat16 [8192, 8192], P('head', 'seq'), may hold values from -0.0625 to 0.0625
- output_down_weight: bfloat16 [8192, 8, 16], P('head'), may hold values from -0.0625 to 0.0625
- output_up_weight: bfloat16 [8, 16, 8192], P(None, None, 'seq'), may hold values from -3.59375 to 3.59375
Outputs:
- handed: bfloat16 [8, 2, 2048, 2, 1024], P(('pool', 'seq'), None, None, None, 'head')
- decoded: bfloat16 [384, 8192], P(('pool', 'head'), 'seq')
The draws below stay inside these ranges and needn't reach their ends.
Inputs may be any that keep to these rules, and one draw needn't show every extreme that they name: `destination`: among one pool's 4 requests no decode owner is named more than 2 times, and some owner exactly 2 times; in each pool owners 0 and 3 both receive requests.
All inputs are finite; a program needn't handle non-finite values.
Results may differ from the reference program's by a relative error of at most 0.0085.
Values may be sent and summed in bfloat16 or wider, within the bound.
A program may use at most 128 MiB of HBM per device.

```python
import jax
import jax.numpy as jnp
from jax import lax

MODEL_DIM = 8192
QUERY_HEADS = 64
KEY_HEADS = 8
HEAD_DIM = 128
ADAPTER_RANK = 16
ADAPTER_COUNT = 8
PROMPT = 2048
CAP = 2
REQ_POOL = 4
ROWS_DEV = 48
CONTEXT_SLOTS = 128
REQS = 8
DECODE_ROWS = 384
DECODERS = 4
OWNERS = 8
N_POOL = 2
N_SEQ = 4


def cache_front(key):
    leading_part = jax.random.normal(jax.random.fold_in(key, 11), (DECODE_ROWS, 2, 2, KEY_HEADS * HEAD_DIM), jnp.float32)
    leading_part = jnp.clip(leading_part, -6.0, 6.0)
    return leading_part


def draw_key_value_cache(key, part):
    leading_part = cache_front(key)
    remaining_part = jax.random.normal(jax.random.fold_in(key, 12), (DECODE_ROWS, CONTEXT_SLOTS - 2, 2, KEY_HEADS * HEAD_DIM), jnp.float32)
    remaining_part = jnp.clip(remaining_part, -6.0, 6.0)
    whole = jnp.concatenate([leading_part, remaining_part], axis=1)
    return jnp.clip(whole, -6.0, 6.0).astype(jnp.bfloat16)


def draw_rotated_query(key, part):
    query_matrix = jax.random.normal(jax.random.fold_in(key, 21), (DECODE_ROWS, QUERY_HEADS * HEAD_DIM), jnp.float32)
    query_matrix = jnp.clip(query_matrix, -5.0, 5.0)
    return query_matrix.astype(jnp.bfloat16)


def draw_destination(key, part):
    halves = []
    for pool_index in range(N_POOL):
        sub_key = jax.random.fold_in(key, 100 + pool_index)
        ranks = jax.random.permutation(jax.random.fold_in(sub_key, 1), N_SEQ).astype(jnp.int32)
        coin = jax.random.randint(jax.random.fold_in(sub_key, 4), (), 0, 2).astype(jnp.int32)
        first_owner = coin * (N_SEQ - 1)
        second_owner = N_SEQ - 1 - first_owner
        ranks = ranks.at[first_owner].set(-2)
        ranks = ranks.at[second_owner].set(-1)
        owners = jnp.argsort(ranks, stable=True).astype(jnp.int32)
        counts = jax.random.randint(jax.random.fold_in(sub_key, 2), (N_SEQ,), 1, CAP + 1)
        counts = counts.at[0].set(CAP)
        listed = jnp.repeat(owners, counts, total_repeat_length=REQ_POOL)
        shuffle = jax.random.permutation(jax.random.fold_in(sub_key, 3), REQ_POOL)
        halves.append(listed[shuffle])
    return jnp.concatenate(halves).astype(jnp.int32)


def place_ends(values, key, smallest, top_value):
    index_at = [jax.random.randint(jax.random.fold_in(key, axis), (), 0, length) for axis, length in enumerate(values.shape)]
    widest = values.shape.index(max(values.shape))
    beside = index_at[:widest] + [(index_at[widest] + 1) % values.shape[widest]] + index_at[widest + 1:]
    return values.at[tuple(index_at)].set(smallest).at[tuple(beside)].set(top_value)


def level_of(rng, dims, pieces, low, largest):
    level = 1.0
    for dim, blocks in pieces:
        heights = jax.random.uniform(jax.random.fold_in(jax.random.fold_in(rng, 6), dim), (blocks,), jnp.float32, low / len(pieces), largest / len(pieces))
        level = level * jnp.repeat(jnp.exp(heights), dims[dim] // blocks).reshape((-1,) + (1,) * (len(dims) - 1 - dim))
    return level


def noise(stream_key, dims, scale, reach, cuts=(), kind=jnp.bfloat16):
    values = jax.random.normal(stream_key, dims, jnp.float32) * scale
    if len(cuts) > 0:
        values = level_of(stream_key, dims, cuts, -0.22, 0.18) * values
    return jnp.clip(values, min=-reach, max=reach).astype(kind)


def setup_inputs(seed: int = 0) -> dict:
    key_of = jax.random.split(jax.random.key(seed), 15)
    prompt = noise(key_of[0], (REQS, PROMPT, MODEL_DIM), 1.0, 6.0, ((0, 2), (1, 4)))
    key_value_weight = noise(key_of[1], (MODEL_DIM, 2, KEY_HEADS * HEAD_DIM), MODEL_DIM ** -0.5, 0.0625, ((0, 4), (2, 4)))
    adapter_down_weight = noise(key_of[2], (MODEL_DIM, ADAPTER_COUNT * 2 * ADAPTER_RANK), MODEL_DIM ** -0.5, 0.0625, ((0, 4),))
    adapter_up_weight = noise(key_of[3], (ADAPTER_COUNT, 2, ADAPTER_RANK, KEY_HEADS * HEAD_DIM), 0.125, 0.75, ((3, 4),))
    request_adapter_index = place_ends(jax.random.randint(key_of[4], (REQS,), 0, ADAPTER_COUNT), jax.random.fold_in(key_of[4], 1), 0, ADAPTER_COUNT - 1).astype(jnp.int32)
    destination = draw_destination(jax.random.fold_in(key_of[14], 71), 0)
    rotated_query = draw_rotated_query(jax.random.fold_in(key_of[14], 71), 0)
    key_value_cache = draw_key_value_cache(jax.random.fold_in(key_of[14], 71), 0)
    current_key_value = noise(key_of[8], (DECODE_ROWS, 2, KEY_HEADS * HEAD_DIM), 1.0, 6.0, ((0, 8), (2, 4)))
    cached_length = place_ends(jax.random.randint(key_of[9], (DECODE_ROWS,), 1, CONTEXT_SLOTS + 1), jax.random.fold_in(key_of[9], 1), 1, CONTEXT_SLOTS).astype(jnp.int32)
    row_adapter_index = place_ends(jax.random.randint(key_of[10], (DECODE_ROWS,), 0, ADAPTER_COUNT), jax.random.fold_in(key_of[10], 1), 0, ADAPTER_COUNT - 1).astype(jnp.int32)
    output_weight = noise(key_of[11], (QUERY_HEADS * HEAD_DIM, MODEL_DIM), (QUERY_HEADS * HEAD_DIM) ** -0.5, 0.0625, ((0, 4), (1, 4)))
    output_down_weight = noise(key_of[12], (QUERY_HEADS * HEAD_DIM, ADAPTER_COUNT, ADAPTER_RANK), (QUERY_HEADS * HEAD_DIM) ** -0.5, 0.0625, ((0, 4),))
    output_up_weight = noise(key_of[13], (ADAPTER_COUNT, ADAPTER_RANK, MODEL_DIM), 0.6, 3.59375, ((2, 4),))
    return {"prompt": prompt, "key_value_weight": key_value_weight, "adapter_down_weight": adapter_down_weight, "adapter_up_weight": adapter_up_weight, "request_adapter_index": request_adapter_index, "destination": destination, "rotated_query": rotated_query, "key_value_cache": key_value_cache, "current_key_value": current_key_value, "cached_length": cached_length, "row_adapter_index": row_adapter_index, "output_weight": output_weight, "output_down_weight": output_down_weight, "output_up_weight": output_up_weight}


def attend_rows(query_matrix, key_value_cache, prefill_state, lengths):
    decode_count = query_matrix.shape[0]
    query_groups = QUERY_HEADS // KEY_HEADS
    query_batch = query_matrix.astype(jnp.float32).reshape(decode_count, KEY_HEADS, query_groups, HEAD_DIM)
    key_matrix = key_value_cache[:, :, 0].astype(jnp.float32).reshape(decode_count, CONTEXT_SLOTS, KEY_HEADS, HEAD_DIM)
    value_matrix = key_value_cache[:, :, 1].astype(jnp.float32).reshape(decode_count, CONTEXT_SLOTS, KEY_HEADS, HEAD_DIM)
    prefill_key = prefill_state[:, 0].astype(jnp.float32).reshape(decode_count, KEY_HEADS, HEAD_DIM)
    prefill_value = prefill_state[:, 1].astype(jnp.float32).reshape(decode_count, KEY_HEADS, HEAD_DIM)
    factor = HEAD_DIM ** -0.5
    scores = jnp.einsum("rkgd,rckd->rkgc", query_batch, key_matrix) * factor
    own_score = jnp.einsum("rkgd,rkd->rkg", query_batch, prefill_key) * factor
    valid = (jnp.arange(CONTEXT_SLOTS, dtype=jnp.int32)[None, :] < lengths[:, None])[:, None, None, :]
    highest = jnp.maximum(jnp.max(jnp.where(valid, scores, -1e30), axis=-1), own_score)
    raw = jnp.where(valid, jnp.exp(scores - highest[..., None]), 0.0)
    own_raw = jnp.exp(own_score - highest)
    normer = jnp.sum(raw, axis=-1) + own_raw
    weights = lax.optimization_barrier((raw / normer[..., None]).astype(jnp.bfloat16)).astype(jnp.float32)
    own_weight = lax.optimization_barrier((own_raw / normer).astype(jnp.bfloat16)).astype(jnp.float32)
    mixed = jnp.einsum("rkgc,rckd->rkgd", weights, value_matrix)
    mixed = mixed + own_weight[..., None] * prefill_value[:, :, None, :]
    return mixed.reshape(decode_count, QUERY_HEADS * HEAD_DIM).astype(jnp.bfloat16)


def reference(prompt, key_value_weight, adapter_down_weight, adapter_up_weight, request_adapter_index, destination, rotated_query, key_value_cache, current_key_value, cached_length, row_adapter_index, output_weight, output_down_weight, output_up_weight):
    key_value_width = KEY_HEADS * HEAD_DIM
    token_matrix = prompt.reshape(REQS * PROMPT, MODEL_DIM)
    base_kv = jnp.dot(token_matrix, key_value_weight.reshape(MODEL_DIM, 2 * key_value_width), preferred_element_type=jnp.float32)
    reduced_everything = jnp.dot(token_matrix, adapter_down_weight, preferred_element_type=jnp.float32)
    reduced_everything = reduced_everything.reshape(REQS, PROMPT, ADAPTER_COUNT, 2, ADAPTER_RANK)
    adapter_selector = request_adapter_index[:, None] == jnp.arange(ADAPTER_COUNT, dtype=jnp.int32)[None, :]
    low_rank = jnp.sum(jnp.where(adapter_selector[:, None, :, None, None], reduced_everything, 0.0), axis=2)
    selected_up_weight = adapter_up_weight.astype(jnp.float32)[request_adapter_index]
    correction = jnp.einsum("rtkq,rkqf->rtkf", low_rank, selected_up_weight, precision=lax.Precision.HIGHEST)
    prefilled = (base_kv.reshape(REQS, PROMPT, 2, key_value_width) + correction).astype(jnp.bfloat16)

    owners = destination.reshape(N_POOL, REQ_POOL)
    order_index = jnp.arange(REQ_POOL, dtype=jnp.int32)
    earlier = (owners[:, :, None] == owners[:, None, :]) & (order_index[None, None, :] < order_index[None, :, None])
    slot_of = jnp.sum(earlier.astype(jnp.int32), axis=2).astype(jnp.int32)
    target_pool = (jnp.arange(N_POOL, dtype=jnp.int32) + 1) % N_POOL
    target = (target_pool[:, None] * DECODERS + owners).reshape(REQS).astype(jnp.int32)
    handed = jnp.zeros((OWNERS, CAP, PROMPT, 2, key_value_width), jnp.bfloat16)
    handed = handed.at[target, slot_of.reshape(REQS)].set(prefilled)

    blocks = DECODE_ROWS // ROWS_DEV

    def one_block(operands):
        return attend_rows(operands[0], operands[1], operands[2], operands[3])

    attended = lax.map(one_block, (rotated_query.reshape(blocks, ROWS_DEV, QUERY_HEADS * HEAD_DIM), key_value_cache.reshape(blocks, ROWS_DEV, CONTEXT_SLOTS, 2, key_value_width), current_key_value.reshape(blocks, ROWS_DEV, 2, key_value_width), cached_length.reshape(blocks, ROWS_DEV)))
    attended = attended.reshape(DECODE_ROWS, QUERY_HEADS * HEAD_DIM)
    low_rows = jnp.dot(attended, output_down_weight.reshape(QUERY_HEADS * HEAD_DIM, ADAPTER_COUNT * ADAPTER_RANK), preferred_element_type=jnp.float32)
    keep = row_adapter_index[:, None] == (jnp.arange(ADAPTER_COUNT * ADAPTER_RANK, dtype=jnp.int32) // ADAPTER_RANK)[None, :]
    low_rows = jnp.where(keep, low_rows, 0.0)
    decoded = jnp.dot(attended, output_weight, preferred_element_type=jnp.float32)
    decoded = decoded + jnp.dot(low_rows, output_up_weight.reshape(ADAPTER_COUNT * ADAPTER_RANK, MODEL_DIM).astype(jnp.float32), precision=lax.Precision.HIGHEST)
    return handed, decoded.astype(jnp.bfloat16)
```

```python
import jax
import jax.numpy as jnp
from jax import lax
from jax.experimental import pallas as pl
from jax.experimental.pallas import tpu as pltpu
from jax.sharding import PartitionSpec as P

HEAD_DIM = 128
ADAPTER_RANK = 16
ADAPTER_COUNT = 8
CAP = 2


def exchanged(value, axis, mask):
    pairs = [(source, source ^ mask) for source in range(lax.axis_size(axis))]
    return lax.ppermute(value, axis, pairs)


def gathered(value, axis):
    size = lax.axis_size(axis)
    index = lax.axis_index(axis)
    held = value[None]
    mask = size // 2
    while mask >= 1:
        other = exchanged(held, axis, mask)
        low_bit = (index // mask) % 2 == 0
        first = jnp.where(low_bit, held, other)
        second = jnp.where(low_bit, other, held)
        held = jnp.stack([first, second], axis=1).reshape((-1,) + value.shape)
        mask //= 2
    return held


def scattered_sum(value, axis):
    size = lax.axis_size(axis)
    index = lax.axis_index(axis)
    held = value.reshape((size, value.shape[0] // size) + value.shape[1:])
    mask = 1
    while mask < size:
        split = held.reshape((held.shape[0] // 2, 2) + held.shape[1:])
        low_bit = (index // mask) % 2 == 0
        keep = jnp.where(low_bit, split[:, 0], split[:, 1])
        give = jnp.where(low_bit, split[:, 1], split[:, 0])
        held = keep + exchanged(give, axis, mask)
        mask *= 2
    return held[0]


def attend_kernel(lengths, query_ref, cache_ref, key_ref, value_ref, out_ref):
    rows, positions = cache_ref.shape[0], cache_ref.shape[1]
    kv_heads = key_ref.shape[1]
    groups = query_ref.shape[1] // kv_heads
    start = pl.program_id(0) * rows
    lane = lax.broadcasted_iota(jnp.int32, (groups, 2 * positions), 1)
    factor = HEAD_DIM ** (-0.5)
    for row in range(rows):
        pairs = cache_ref[row].reshape(2 * positions, kv_heads * HEAD_DIM)
        length = lengths[start + row]
        valid = (lane % 2 == 0) & (lane < 2 * length)
        for head in range(kv_heads):
            block = pairs[:, head * HEAD_DIM : (head + 1) * HEAD_DIM]
            query = query_ref[row, head * groups : (head + 1) * groups, :]
            own_key = key_ref[row, head : head + 1, :].astype(jnp.float32)
            own_value = value_ref[row, head : head + 1, :].astype(jnp.float32)
            scores = (
                lax.dot_general(
                    query, block, (((1,), (1,)), ((), ())), preferred_element_type=jnp.float32
                )
                * factor
            )
            own = jnp.sum(query.astype(jnp.float32) * own_key, axis=1, keepdims=True) * factor
            highest = jnp.maximum(
                jnp.max(jnp.where(valid, scores, -1e30), axis=1, keepdims=True), own
            )
            raw = jnp.where(valid, jnp.exp(scores - highest), 0.0)
            own_raw = jnp.exp(own - highest)
            total = jnp.sum(raw, axis=1, keepdims=True) + own_raw
            weights = pltpu.roll(raw / total, 1, 1).astype(jnp.bfloat16)
            own_weight = (own_raw / total).astype(jnp.bfloat16).astype(jnp.float32)
            mixed = jnp.dot(weights, block, preferred_element_type=jnp.float32)
            out_ref[row, head * groups : (head + 1) * groups, :] = (
                mixed + own_weight * own_value
            ).astype(jnp.bfloat16)


def attend(query, cache, current, lengths):
    rows, positions, _, width = cache.shape
    kv_heads = width // HEAD_DIM
    heads = query.shape[1] // HEAD_DIM
    step = next(size for size in (8, 4, 2, 1) if rows % size == 0)
    query = query.reshape(rows, heads, HEAD_DIM)
    own_key = current[:, 0].reshape(rows, kv_heads, HEAD_DIM)
    own_value = current[:, 1].reshape(rows, kv_heads, HEAD_DIM)
    out = pl.pallas_call(
        attend_kernel,
        grid_spec=pltpu.PrefetchScalarGridSpec(
            num_scalar_prefetch=1,
            grid=(rows // step,),
            in_specs=[
                pl.BlockSpec((step, heads, HEAD_DIM), lambda i, _: (i, 0, 0)),
                pl.BlockSpec((step, positions, 2, width), lambda i, _: (i, 0, 0, 0)),
                pl.BlockSpec((step, kv_heads, HEAD_DIM), lambda i, _: (i, 0, 0)),
                pl.BlockSpec((step, kv_heads, HEAD_DIM), lambda i, _: (i, 0, 0)),
            ],
            out_specs=pl.BlockSpec((step, heads, HEAD_DIM), lambda i, _: (i, 0, 0)),
        ),
        out_shape=jax.ShapeDtypeStruct((rows, heads, HEAD_DIM), jnp.bfloat16),
        cost_estimate=pl.CostEstimate(
            flops=8 * rows * heads * positions * HEAD_DIM,
            bytes_accessed=4 * rows * positions * width,
            transcendentals=2 * rows * heads * positions,
        ),
    )(lengths, query, cache, own_key, own_value)
    return out.reshape(rows, heads * HEAD_DIM)


def weave_kernel(key_ref, value_ref, out_ref):
    tokens, width = key_ref.shape[2], key_ref.shape[3]
    part = 128
    row = lax.broadcasted_iota(jnp.int32, (2 * part, 2 * part), 0)
    column = lax.broadcasted_iota(jnp.int32, (2 * part, 2 * part), 1)
    order = jnp.where(column == (row % 2) * part + row // 2, 1.0, 0.0).astype(jnp.bfloat16)
    for at in range(0, tokens, part):
        both = jnp.concatenate(
            [key_ref[0, 0, at : at + part, :], value_ref[0, 0, at : at + part, :]], axis=0
        )
        woven = jnp.dot(order, both, preferred_element_type=jnp.float32).astype(jnp.bfloat16)
        out_ref[0, 0, at : at + part, :, :] = woven.reshape(part, 2, width)


def weave(keys, values):
    sources, slots, tokens, width = keys.shape
    spec = pl.BlockSpec((1, 1, tokens, width), lambda slot, source: (source, slot, 0, 0))
    return pl.pallas_call(
        weave_kernel,
        grid=(slots, sources),
        in_specs=[spec, spec],
        out_specs=pl.BlockSpec(
            (1, 1, tokens, 2, width), lambda slot, source: (0, slot, source, 0, 0)
        ),
        out_shape=jax.ShapeDtypeStruct((1, slots, sources * tokens, 2, width), jnp.bfloat16),
        cost_estimate=pl.CostEstimate(
            flops=1024 * slots * sources * tokens * width,
            bytes_accessed=8 * slots * sources * tokens * width,
            transcendentals=0,
        ),
    )(keys, values)


def slot_hits(owners, decoders):
    requests = owners.shape[0]
    order = jnp.arange(requests, dtype=jnp.int32)
    same = owners[:, None] == owners[None, :]
    slot_of = jnp.sum((same & (order[None, :] < order[:, None])).astype(jnp.int32), axis=1)
    slot_hit = slot_of[None, :] == jnp.arange(CAP, dtype=jnp.int32)[:, None]
    owner_hit = owners[None, :] == jnp.arange(decoders, dtype=jnp.int32)[:, None]
    return owner_hit[:, None, :] & slot_hit[None, :, :]


def hand_over(block, hits):
    arrived = exchanged(block, "pool", 1)
    outgoing = jnp.zeros(hits.shape[:2] + block.shape[1:], block.dtype)
    for request in range(block.shape[0]):
        outgoing = jnp.where(
            hits[:, :, request][:, :, None, None], arrived[request][None, None], outgoing
        )
    return lax.all_to_all(outgoing, "seq", split_axis=0, concat_axis=0, tiled=True)


def body(
    prompt,
    key_value_weight,
    adapter_down_weight,
    adapter_up_weight,
    request_adapter_index,
    destination,
    rotated_query,
    key_value_cache,
    current_key_value,
    cached_length,
    row_adapter_index,
    output_weight,
    output_down_weight,
    output_up_weight,
):
    requests, tok_dev, model_width = prompt.shape
    width = key_value_weight.shape[2]
    shard = key_value_weight.shape[0]
    decoders = lax.axis_size("seq")
    heads = lax.axis_size("head")
    columns = 2 * ADAPTER_RANK
    tokens = prompt.reshape(requests * tok_dev, model_width)

    share = requests // heads if requests % heads == 0 else requests
    mine = lax.axis_index("head") * share if share < requests else 0
    my_adapter = lax.dynamic_slice_in_dim(request_adapter_index, mine, share)
    column = jnp.arange(ADAPTER_COUNT * columns, dtype=jnp.int32)
    wanted = my_adapter[:, None] * columns + jnp.arange(columns, dtype=jnp.int32)[None, :]
    pick = (wanted.reshape(-1)[:, None] == column[None, :]).astype(jnp.bfloat16)
    down = lax.dot_general(
        pick, adapter_down_weight, (((1,), (1,)), ((), ())), preferred_element_type=jnp.float32
    ).astype(jnp.bfloat16)
    matrix = key_value_weight.reshape(shard, 2 * width)
    down_all = gathered(down, "seq")
    key_all = gathered(matrix[:, :width], "seq").reshape(model_width, width)
    value_all = gathered(matrix[:, width:], "seq").reshape(model_width, width)

    attended = attend(rotated_query, key_value_cache, current_key_value, cached_length)
    attn_rows = gathered(attended, "seq").reshape(-1, attended.shape[1])
    ranks = ADAPTER_COUNT * ADAPTER_RANK
    down_flat = output_down_weight.reshape(output_down_weight.shape[0], ranks)
    up_flat = output_up_weight.reshape(ranks, output_up_weight.shape[2])
    rank_owner = jnp.arange(ranks, dtype=jnp.int32) // ADAPTER_RANK
    low_rows = jnp.dot(attn_rows, down_flat, preferred_element_type=jnp.float32)
    low_rows = jnp.where(row_adapter_index[:, None] == rank_owner[None, :], low_rows, 0.0)
    terms = jnp.dot(attn_rows, output_weight, preferred_element_type=jnp.float32)
    terms = terms + jnp.dot(
        low_rows.astype(jnp.bfloat16), up_flat, preferred_element_type=jnp.float32
    )
    decoded = scattered_sum(terms, "head").astype(jnp.bfloat16)

    my_tokens = lax.dynamic_slice_in_dim(prompt, mine, share, axis=0)
    my_down = down_all.transpose(1, 0, 2).reshape(share, columns, model_width)
    my_low = jnp.einsum("rtk,rck->rct", my_tokens, my_down, preferred_element_type=jnp.float32)
    low = gathered(my_low, "head") if share < requests else my_low[None]
    low = low.reshape(requests, 2, ADAPTER_RANK, tok_dev).astype(jnp.bfloat16)
    own = jnp.eye(requests, dtype=jnp.bool_)[None, :, None, :, None]
    spread = jnp.where(
        own, low.transpose(1, 0, 2, 3)[:, :, :, None, :], jnp.zeros((), jnp.bfloat16)
    ).reshape(2, requests * ADAPTER_RANK, requests * tok_dev)
    selector = request_adapter_index[:, None] == jnp.arange(ADAPTER_COUNT, dtype=jnp.int32)[None, :]
    up = jnp.einsum(
        "um,mdzt->duzt",
        selector.astype(jnp.bfloat16),
        adapter_up_weight,
        preferred_element_type=jnp.float32,
    ).astype(jnp.bfloat16)
    up = up.reshape(2, requests * ADAPTER_RANK, width)

    pool_index = lax.axis_index("pool")
    other_owners = lax.dynamic_slice_in_dim(destination, (1 - pool_index) * requests, requests)
    hits = slot_hits(other_owners, decoders)

    handed = []
    for which, weight in enumerate((key_all, value_all)):
        base = jnp.dot(tokens, weight, preferred_element_type=jnp.float32)
        extra = lax.dot_general(
            spread[which], up[which], (((0,), (0,)), ((), ())), preferred_element_type=jnp.float32
        )
        block = (base + extra).astype(jnp.bfloat16).reshape(requests, tok_dev, width)
        handed.append(hand_over(block, hits))
    return (weave(handed[0], handed[1]), decoded)


def solution(mesh):
    in_specs = (
        P("pool", "seq", None),
        P("seq", None, "head"),
        P("seq", None),
        P(None, None, None, "head"),
        P("pool"),
        P(),
        P(("pool", "seq"), "head"),
        P(("pool", "seq"), None, None, "head"),
        P(("pool", "seq"), None, "head"),
        P(("pool", "seq")),
        P("pool"),
        P("head", "seq"),
        P("head", None, None),
        P(None, None, "seq"),
    )
    out_specs = (P(("pool", "seq"), None, None, None, "head"), P(("pool", "head"), "seq"))
    return jax.shard_map(body, mesh=mesh, in_specs=in_specs, out_specs=out_specs, check_vma=False)
```

```python
import jax
import jax.numpy as jnp
from jax import lax
from jax.experimental import pallas as pl
from jax.experimental.pallas import tpu as pltpu
from jax.sharding import PartitionSpec as P

HEAD_DIM = 128
ADAPTER_RANK = 16
ADAPTER_COUNT = 8
CAP = 2


def exchanged(value, axis, mask):
    pairs = [(source, source ^ mask) for source in range(lax.axis_size(axis))]
    return lax.ppermute(value, axis, pairs)


def gathered(value, axis, after=None):
    size = lax.axis_size(axis)
    index = lax.axis_index(axis)
    held = value[None]
    mask = size // 2
    arrived = None
    while mask >= 1:
        other = exchanged(held, axis, mask)
        if after is not None:
            other = lax.optimization_barrier((other, after))[0]
        arrived = other if arrived is None else arrived
        low_bit = (index // mask) % 2 == 0
        first = jnp.where(low_bit, held, other)
        second = jnp.where(low_bit, other, held)
        held = jnp.stack([first, second], axis=1).reshape((-1,) + value.shape)
        mask //= 2
    return held, arrived


def scattered_sum(value, axis):
    size = lax.axis_size(axis)
    index = lax.axis_index(axis)
    held = value.reshape((size, value.shape[0] // size) + value.shape[1:])
    mask = 1
    while mask < size:
        split = held.reshape((held.shape[0] // 2, 2) + held.shape[1:])
        low_bit = (index // mask) % 2 == 0
        keep = jnp.where(low_bit, split[:, 0], split[:, 1])
        give = jnp.where(low_bit, split[:, 1], split[:, 0])
        held = keep + exchanged(give, axis, mask)
        mask *= 2
    return held[0]


def attend_kernel(lengths, query_ref, cache_ref, key_ref, value_ref, out_ref):
    rows, positions = cache_ref.shape[0], cache_ref.shape[1]
    kv_heads = key_ref.shape[1]
    groups = query_ref.shape[1] // kv_heads
    start = pl.program_id(0) * rows
    lane = lax.broadcasted_iota(jnp.int32, (groups, 2 * positions), 1)
    factor = HEAD_DIM ** (-0.5)
    blocks, scores, owns = [], [], []
    for row in range(rows):
        pairs = cache_ref[row].reshape(2 * positions, kv_heads * HEAD_DIM)
        valid = (lane % 2 == 0) & (lane < 2 * lengths[start + row])
        for head in range(kv_heads):
            block = pairs[:, head * HEAD_DIM : (head + 1) * HEAD_DIM]
            query = query_ref[row, head * groups : (head + 1) * groups, :]
            own_key = key_ref[row, head : head + 1, :].astype(jnp.float32)
            own = jnp.sum(query.astype(jnp.float32) * own_key, axis=1, keepdims=True) * factor
            score = lax.dot_general(
                query, block, (((1,), (1,)), ((), ())), preferred_element_type=jnp.float32
            )
            blocks.append(block)
            scores.append(jnp.where(valid, score * factor, -1e30))
            owns.append(own)
    scores = jnp.concatenate(scores, axis=0)
    own = jnp.concatenate(owns, axis=0)
    highest = jnp.maximum(jnp.max(scores, axis=1, keepdims=True), own)
    raw = jnp.where(scores > -1e29, jnp.exp(scores - highest), 0.0)
    own_raw = jnp.exp(own - highest)
    total = jnp.sum(raw, axis=1, keepdims=True) + own_raw
    weights = pltpu.roll(raw / total, 1, 1).astype(jnp.bfloat16)
    own_weight = (own_raw / total).astype(jnp.bfloat16).astype(jnp.float32)
    for row in range(rows):
        for head in range(kv_heads):
            at = (row * kv_heads + head) * groups
            own_value = value_ref[row, head : head + 1, :].astype(jnp.float32)
            mixed = jnp.dot(
                weights[at : at + groups],
                blocks[row * kv_heads + head],
                preferred_element_type=jnp.float32,
            )
            out_ref[row, head * groups : (head + 1) * groups, :] = (
                mixed + own_weight[at : at + groups] * own_value
            ).astype(jnp.bfloat16)


def attend(query, cache, current, lengths):
    rows, positions, _, width = cache.shape
    kv_heads = width // HEAD_DIM
    heads = query.shape[1] // HEAD_DIM
    step = next(size for size in (8, 4, 2, 1) if rows % size == 0)
    query = query.reshape(rows, heads, HEAD_DIM)
    own_key = current[:, 0].reshape(rows, kv_heads, HEAD_DIM)
    own_value = current[:, 1].reshape(rows, kv_heads, HEAD_DIM)
    out = pl.pallas_call(
        attend_kernel,
        grid_spec=pltpu.PrefetchScalarGridSpec(
            num_scalar_prefetch=1,
            grid=(rows // step,),
            in_specs=[
                pl.BlockSpec((step, heads, HEAD_DIM), lambda i, _: (i, 0, 0)),
                pl.BlockSpec((step, positions, 2, width), lambda i, _: (i, 0, 0, 0)),
                pl.BlockSpec((step, kv_heads, HEAD_DIM), lambda i, _: (i, 0, 0)),
                pl.BlockSpec((step, kv_heads, HEAD_DIM), lambda i, _: (i, 0, 0)),
            ],
            out_specs=pl.BlockSpec((step, heads, HEAD_DIM), lambda i, _: (i, 0, 0)),
        ),
        out_shape=jax.ShapeDtypeStruct((rows, heads, HEAD_DIM), jnp.bfloat16),
        cost_estimate=pl.CostEstimate(
            flops=8 * rows * heads * positions * HEAD_DIM,
            bytes_accessed=4 * rows * positions * width,
            transcendentals=2 * rows * heads * positions,
        ),
    )(lengths, query, cache, own_key, own_value)
    return out.reshape(rows, heads * HEAD_DIM)


def weave_kernel(key_ref, value_ref, out_ref):
    tokens, width = key_ref.shape[2], key_ref.shape[3]
    part = 128
    row = lax.broadcasted_iota(jnp.int32, (2 * part, 2 * part), 0)
    column = lax.broadcasted_iota(jnp.int32, (2 * part, 2 * part), 1)
    order = jnp.where(column == (row % 2) * part + row // 2, 1.0, 0.0).astype(jnp.bfloat16)
    for at in range(0, tokens, part):
        both = jnp.concatenate(
            [key_ref[0, 0, at : at + part, :], value_ref[0, 0, at : at + part, :]], axis=0
        )
        woven = jnp.dot(order, both, preferred_element_type=jnp.float32).astype(jnp.bfloat16)
        out_ref[0, 0, at : at + part, :, :] = woven.reshape(part, 2, width)


def weave(keys, values):
    sources, slots, tokens, width = keys.shape
    spec = pl.BlockSpec((1, 1, tokens, width), lambda slot, source: (source, slot, 0, 0))
    return pl.pallas_call(
        weave_kernel,
        grid=(slots, sources),
        in_specs=[spec, spec],
        out_specs=pl.BlockSpec(
            (1, 1, tokens, 2, width), lambda slot, source: (0, slot, source, 0, 0)
        ),
        out_shape=jax.ShapeDtypeStruct((1, slots, sources * tokens, 2, width), jnp.bfloat16),
        cost_estimate=pl.CostEstimate(
            flops=1024 * slots * sources * tokens * width,
            bytes_accessed=8 * slots * sources * tokens * width,
            transcendentals=0,
        ),
    )(keys, values)


def slot_hits(owners, decoders):
    requests = owners.shape[0]
    order = jnp.arange(requests, dtype=jnp.int32)
    same = owners[:, None] == owners[None, :]
    slot_of = jnp.sum((same & (order[None, :] < order[:, None])).astype(jnp.int32), axis=1)
    slot_hit = slot_of[None, :] == jnp.arange(CAP, dtype=jnp.int32)[:, None]
    owner_hit = owners[None, :] == jnp.arange(decoders, dtype=jnp.int32)[:, None]
    return owner_hit[:, None, :] & slot_hit[None, :, :]


def hand_over(arrived, hits, after):
    if after is not None:
        arrived = lax.optimization_barrier((arrived, after))[0]
    outgoing = jnp.zeros(hits.shape[:2] + arrived.shape[1:], arrived.dtype)
    for request in range(arrived.shape[0]):
        outgoing = jnp.where(
            hits[:, :, request][:, :, None, None], arrived[request][None, None], outgoing
        )
    landed = lax.all_to_all(outgoing, "seq", split_axis=0, concat_axis=0, tiled=True)
    return landed, outgoing


def body(
    prompt,
    key_value_weight,
    adapter_down_weight,
    adapter_up_weight,
    request_adapter_index,
    destination,
    rotated_query,
    key_value_cache,
    current_key_value,
    cached_length,
    row_adapter_index,
    output_weight,
    output_down_weight,
    output_up_weight,
):
    requests, tok_dev, model_width = prompt.shape
    width = key_value_weight.shape[2]
    shard = key_value_weight.shape[0]
    decoders = lax.axis_size("seq")
    heads = lax.axis_size("head")
    columns = 2 * ADAPTER_RANK
    tokens = prompt.reshape(requests * tok_dev, model_width)

    share = requests // heads if requests % heads == 0 else requests
    mine = lax.axis_index("head") * share if share < requests else 0
    my_adapter = lax.dynamic_slice_in_dim(request_adapter_index, mine, share)
    column = jnp.arange(ADAPTER_COUNT * columns, dtype=jnp.int32)
    wanted = my_adapter[:, None] * columns + jnp.arange(columns, dtype=jnp.int32)[None, :]
    pick = (wanted.reshape(-1)[:, None] == column[None, :]).astype(jnp.bfloat16)
    down = lax.dot_general(
        pick, adapter_down_weight, (((1,), (1,)), ((), ())), preferred_element_type=jnp.float32
    ).astype(jnp.bfloat16)
    matrix = key_value_weight.reshape(shard, 2 * width)
    down_all, down_first = gathered(down, "seq")
    matrix = lax.optimization_barrier((matrix, down_first))[0]
    key_all, key_first = gathered(matrix[:, :width], "seq")
    value_all, _ = gathered(matrix[:, width:], "seq", key_all)
    key_all = key_all.reshape(model_width, width)
    value_all = value_all.reshape(model_width, width)
    rotated_query = lax.optimization_barrier((rotated_query, key_first))[0]

    attended = attend(rotated_query, key_value_cache, current_key_value, cached_length)
    attn_rows = gathered(attended, "seq")[0].reshape(-1, attended.shape[1])
    ranks = ADAPTER_COUNT * ADAPTER_RANK
    down_flat = output_down_weight.reshape(output_down_weight.shape[0], ranks)
    up_flat = output_up_weight.reshape(ranks, output_up_weight.shape[2])
    rank_owner = jnp.arange(ranks, dtype=jnp.int32) // ADAPTER_RANK
    low_rows = jnp.dot(attn_rows, down_flat, preferred_element_type=jnp.float32)
    low_rows = jnp.where(row_adapter_index[:, None] == rank_owner[None, :], low_rows, 0.0)
    terms = jnp.dot(attn_rows, output_weight, preferred_element_type=jnp.float32)
    terms = terms + jnp.dot(
        low_rows.astype(jnp.bfloat16), up_flat, preferred_element_type=jnp.float32
    )
    decoded = scattered_sum(terms, "head").astype(jnp.bfloat16)

    my_tokens = lax.dynamic_slice_in_dim(prompt, mine, share, axis=0)
    my_down = down_all.transpose(1, 0, 2).reshape(share, columns, model_width)
    my_low = jnp.einsum("rtk,rck->rct", my_tokens, my_down, preferred_element_type=jnp.float32)
    low = gathered(my_low, "head")[0] if share < requests else my_low[None]
    low = low.reshape(requests, 2, ADAPTER_RANK, tok_dev).astype(jnp.bfloat16)
    own = jnp.eye(requests, dtype=jnp.bool_)[None, :, None, :, None]
    spread = jnp.where(
        own, low.transpose(1, 0, 2, 3)[:, :, :, None, :], jnp.zeros((), jnp.bfloat16)
    ).reshape(2, requests * ADAPTER_RANK, requests * tok_dev)
    selector = request_adapter_index[:, None] == jnp.arange(ADAPTER_COUNT, dtype=jnp.int32)[None, :]
    up = jnp.einsum(
        "um,mdzt->duzt",
        selector.astype(jnp.bfloat16),
        adapter_up_weight,
        preferred_element_type=jnp.float32,
    ).astype(jnp.bfloat16)
    up = up.reshape(2, requests * ADAPTER_RANK, width)

    pool_index = lax.axis_index("pool")
    other_owners = lax.dynamic_slice_in_dim(destination, (1 - pool_index) * requests, requests)
    hits = slot_hits(other_owners, decoders)

    arrived = []
    for which, weight in enumerate((key_all, value_all)):
        base = jnp.dot(tokens, weight, preferred_element_type=jnp.float32)
        extra = lax.dot_general(
            spread[which], up[which], (((0,), (0,)), ((), ())), preferred_element_type=jnp.float32
        )
        block = (base + extra).astype(jnp.bfloat16).reshape(requests, tok_dev, width)
        arrived.append(exchanged(block, "pool", 1))
    handed, outgoing = [], block
    for blocks in arrived:
        landed, outgoing = hand_over(blocks, hits, outgoing)
        handed.append(landed)
    return (weave(handed[0], handed[1]), decoded)


def solution(mesh):
    in_specs = (
        P("pool", "seq", None),
        P("seq", None, "head"),
        P("seq", None),
        P(None, None, None, "head"),
        P("pool"),
        P(),
        P(("pool", "seq"), "head"),
        P(("pool", "seq"), None, None, "head"),
        P(("pool", "seq"), None, "head"),
        P(("pool", "seq")),
        P("pool"),
        P("head", "seq"),
        P("head", None, None),
        P(None, None, "seq"),
    )
    out_specs = (P(("pool", "seq"), None, None, None, "head"), P(("pool", "head"), "seq"))
    return jax.shard_map(body, mesh=mesh, in_specs=in_specs, out_specs=out_specs, check_vma=False)
```
